16 devices in a mesh: dp: 4 (over z, y), pp: 4 (over x, core).
Axes of the slice: x: 2, y: 2, z: 2, core: 2. Of those that a mesh axis runs over, the one named last changes fastest.
Arguments:
- x: bfloat16 [8, 2048, 1024], P(None, 'dp')
- t: bfloat16 [8, 2048, 1024], P(None, 'dp')
- w1: bfloat16 [4, 2, 1024, 4096], P('pp')
- w2: bfloat16 [4, 2, 4096, 1024], P('pp')
Outputs:
- output 1: float32 [4, 2, 1024, 4096], P('pp')
- output 2: float32 [4, 2, 4096, 1024], P('pp')
- output 3: float32 [], replicated
All inputs are finite; a program needn't handle non-finite values.
Results may differ from the reference program's by a relative error of at most 0.00234028.
Values are sent between devices in bfloat16 or wider.
A program may use at most 1 GiB of HBM per device.

```python
import math
import jax
import jax.numpy as jnp
from jax import lax

D = 1024
FF = 4096
STAGES = 4
MICRO = 8
TOKENS = 2048


def _gelu(u):
    c = math.sqrt(2.0 / math.pi)
    return 0.5 * u * (1.0 + jnp.tanh(c * (u + 0.044715 * u * u * u)))


def _dgelu(u):
    c = math.sqrt(2.0 / math.pi)
    th = jnp.tanh(c * (u + 0.044715 * u * u * u))
    return 0.5 * (1.0 + th) + 0.5 * u * (1.0 - th * th) * c * (1.0 + 3.0 * 0.044715 * u * u)


def setup_inputs(seed: int = 0) -> dict:
    k = jax.random.split(jax.random.PRNGKey(seed), 4)
    x = jax.random.normal(k[0], (MICRO, TOKENS, D), jnp.float32)
    t = jax.random.normal(k[1], (MICRO, TOKENS, D), jnp.float32)
    w1 = jax.random.normal(k[2], (STAGES, 2, D, FF), jnp.float32) * D ** -0.5
    w2 = jax.random.normal(k[3], (STAGES, 2, FF, D), jnp.float32) * (FF * STAGES) ** -0.5
    return {'x': x.astype(jnp.bfloat16), 't': t.astype(jnp.bfloat16),
            'w1': w1.astype(jnp.bfloat16), 'w2': w2.astype(jnp.bfloat16)}


def reference(x, t, w1, w2):
    nl = STAGES * 2
    w1f = w1.reshape(nl, D, FF)
    w2f = w2.reshape(nl, FF, D)
    inv = 1.0 / (MICRO * TOKENS * D)

    def fwd(h, w):
        a1, a2 = w
        u = jnp.dot(h, a1, preferred_element_type=jnp.float32).astype(jnp.bfloat16)
        a = _gelu(u.astype(jnp.float32)).astype(jnp.bfloat16)
        h2 = (h.astype(jnp.float32) + jnp.dot(a, a2, preferred_element_type=jnp.float32)).astype(jnp.bfloat16)
        return h2, (h, u)

    def bwd(g, z):
        h, u, a1, a2 = z
        uf = u.astype(jnp.float32)
        a = _gelu(uf).astype(jnp.bfloat16)
        q = jnp.dot(g, a2.T, preferred_element_type=jnp.float32)
        e = (_dgelu(uf) * q).astype(jnp.bfloat16)
        d2 = jnp.dot(a.T, g, preferred_element_type=jnp.float32)
        d1 = jnp.dot(h.T, e, preferred_element_type=jnp.float32)
        g2 = (g.astype(jnp.float32) + jnp.dot(e, a1.T, preferred_element_type=jnp.float32)).astype(jnp.bfloat16)
        return g2, (d1, d2)

    def micro(carry, xt):
        dw1, dw2, loss = carry
        xm, tm = xt
        y, (hs, us) = lax.scan(fwd, xm, (w1f, w2f))
        r = y.astype(jnp.float32) - tm.astype(jnp.float32)
        loss = loss + 0.5 * jnp.sum(r * r) * inv
        g = (r * inv).astype(jnp.bfloat16)
        _, (d1, d2) = lax.scan(bwd, g, (hs, us, w1f, w2f), reverse=True)
        return (dw1 + d1, dw2 + d2, loss), None

    init = (jnp.zeros((nl, D, FF), jnp.float32), jnp.zeros((nl, FF, D), jnp.float32),
            jnp.zeros((), jnp.float32))
    (dw1, dw2, loss), _ = lax.scan(micro, init, (x, t))
    return dw1.reshape(STAGES, 2, D, FF), dw2.reshape(STAGES, 2, FF, D), loss
```

```python
import functools
import math

import jax
import jax.numpy as jnp
from jax import lax
from jax.experimental import pallas as pl
from jax.experimental.pallas import tpu as pltpu
from jax.sharding import PartitionSpec as P

MESH = pl.DeviceIdType.MESH
F32 = jnp.float32
BF16 = jnp.bfloat16
VMEM_LIMIT = 67_043_328
C0 = math.sqrt(2.0 / math.pi)
C1 = 0.044715

D = 1024
FF = 4096
R = 256
NK = 16
FC = 512
TOK = R * NK

BC = 256
NB = FF // BC
HB = BC // 2
TC = 1024
NQ = 2 * TOK // TC

NT = (((1,), (1,)), ((), ()))


def _dot(a, b):
    return jnp.dot(a, b, preferred_element_type=F32)


def _dot_t(a, b):
    return lax.dot_general(a, b, NT, preferred_element_type=F32)


def _act(u):
    t2 = u * u
    th = jnp.tanh(u * (C0 + (C0 * C1) * t2))
    return th, 0.5 * u, t2


def _gelu(u):
    th, hu, _ = _act(u)
    return hu + hu * th


def _dgelu(th, hu, t2):
    return (0.5 + 0.5 * th) + (hu * (1.0 - th * th)) * (C0 + (3.0 * C0 * C1) * t2)


def _pipe_kernel(inv, x, t, w1, w2, hl, gl, wl1, wl2, us, lo,
                 W1, W2, hin, gin, ub, ab, hgb, hop, tb,
                 sw, sx, sg, st, su, sh0, sg2, shg, sop, lh, lg, swl, rwl):
    e = lax.axis_index('dp')
    s = lax.axis_index('pp')
    c = s % 2
    xx = s // 2
    slot = e % 2
    tcore = 2 * xx + e // 2
    first = s == 0
    last = s == 3

    def wcopy(j, i):
        if i == 0:
            return pltpu.make_async_copy(w1.at[j], W1.at[j], sw.at[2 * j])
        return pltpu.make_async_copy(w2.at[j], W2.at[j], sw.at[2 * j + 1])

    for j in range(2):
        for i in range(2):
            wcopy(j, i).start()

    def xcopy(k):
        return pltpu.make_async_copy(x.at[k // 2, pl.ds(pl.multiple_of((k % 2) * R, R), R)], hin.at[k], sx.at[k])

    @pl.when(first)
    def _():
        lax.fori_loop(0, NK, lambda k, z: (xcopy(k).start(), z)[1], 0)

    def wl_copy(i):
        src, dst = ((w1, wl1), (w2, wl2))[i]
        return pltpu.make_async_remote_copy(src.at[e % 2], dst, swl.at[i], rwl.at[i],
                                            device_id=(e, 2 * xx + 1 - c), device_id_type=MESH)

    @pl.when(c == e // 2)
    def _():
        for i in range(2):
            wl_copy(i).start()

    lo[...] = jnp.zeros_like(lo)

    def rows(k):
        return pl.ds(pl.multiple_of(k * R, R), R)

    def ship(src, dst, k, j, sem, land):
        d = 2 * c + j

        @pl.when(d == e)
        def _():
            pltpu.make_async_copy(src, dst.at[slot, rows(k)], sem).start()

        @pl.when(d != e)
        def _():
            pltpu.make_async_remote_copy(src, dst.at[slot, rows(k)], sem, land.at[slot],
                                         device_id=(d, tcore), device_id_type=MESH).start()

    def tile_wait(buf, sem):
        pltpu.make_async_copy(buf, hl.at[0, pl.ds(0, R)], sem).wait()

    def fwd(k, z):
        h4 = k % 4
        h2 = k % 2
        pltpu.make_async_copy(hl.at[0, pl.ds(0, R)], hin.at[k], sx.at[k]).wait()
        ship(hin.at[k], hl, k, 0, sh0, lh)

        @pl.when(last)
        def _():
            pltpu.make_async_copy(t.at[k // 2, pl.ds(pl.multiple_of((k % 2) * R, R), R)], tb, st).start()

        def layer(h, j):
            @pl.when(k == 0)
            def _():
                wcopy(j, 0).wait()
                wcopy(j, 1).wait()

            @pl.when(k > 0)
            def _():
                pltpu.make_async_copy(ub.at[j], us.at[j, k - 1], su.at[j]).wait()

            for f in range(FF // FC):
                cs = slice(f * FC, (f + 1) * FC)
                u = _dot(h, W1[j, :, cs]).astype(BF16)
                ub[j, :, cs] = u
                ab[:, cs] = _gelu(u.astype(F32)).astype(BF16)
            acc = _dot(ab[...], W2[j])
            out = (h.astype(F32) + acc).astype(BF16)
            pltpu.make_async_copy(ub.at[j], us.at[j, k], su.at[j]).start()
            return out

        h1 = layer(hin[k], 0)

        @pl.when(k >= 4)
        def _():
            tile_wait(hgb.at[h4], shg.at[h4])
        hgb[h4] = h1
        y = layer(hgb[h4], 1)
        ship(hgb.at[h4], hl, k, 1, shg.at[h4], lh)

        @pl.when(jnp.logical_and(k >= 2, s < 3))
        def _():
            tile_wait(hop.at[h2], sop.at[h2])
        hop[h2] = y

        @pl.when(s < 3)
        def _():
            pltpu.make_async_remote_copy(hop.at[h2], hin.at[k], sop.at[h2], sx.at[k],
                                         device_id=(e, s + 1), device_id_type=MESH).start()

        @pl.when(last)
        def _():
            pltpu.make_async_copy(t.at[0, pl.ds(0, R)], tb, st).wait()
            r = hop[h2].astype(F32) - tb[...].astype(F32)
            lo[...] += jnp.sum((r * r).reshape(R // 8, 8, D), axis=0)
            gin[k] = (r * inv).astype(BF16)
        return z

    lax.fori_loop(0, NK, fwd, 0)

    for j in range(2):
        pltpu.make_async_copy(ub.at[j], us.at[j, NK - 1], su.at[j]).wait()
        pltpu.make_async_copy(us.at[j, 0], ub.at[j], su.at[j]).start()

    def bwd(k, z):
        h4 = k % 4
        h2 = k % 2

        @pl.when(s < 3)
        def _():
            pltpu.make_async_copy(hl.at[0, pl.ds(0, R)], gin.at[k], sg.at[k]).wait()
        ship(gin.at[k], gl, k, 1, sg2, lg)

        def layer(g, j):
            pltpu.make_async_copy(us.at[j, k], ub.at[j], su.at[j]).wait()
            for f in range(FF // FC):
                cs = slice(f * FC, (f + 1) * FC)
                q = _dot_t(g, W2[j, cs, :])
                th, hu, t2 = _act(ub[j, :, cs].astype(F32))
                ab[:, cs] = (_dgelu(th, hu, t2) * q).astype(BF16)
            acc = _dot_t(ab[...], W1[j])
            out = (g.astype(F32) + acc).astype(BF16)

            @pl.when(k < NK - 1)
            def _():
                pltpu.make_async_copy(us.at[j, k + 1], ub.at[j], su.at[j]).start()
            return out

        g1 = layer(gin[k], 1)
        tile_wait(hgb.at[h4], shg.at[h4])
        hgb[h4] = g1

        @pl.when(s > 0)
        def _():
            g0 = layer(hgb[h4], 0)

            @pl.when(jnp.logical_or(k >= 2, s < 3))
            def _():
                tile_wait(hop.at[h2], sop.at[h2])
            hop[h2] = g0
            pltpu.make_async_remote_copy(hop.at[h2], gin.at[k], sop.at[h2], sg.at[k],
                                         device_id=(e, s - 1), device_id_type=MESH).start()
        ship(hgb.at[h4], gl, k, 0, shg.at[h4], lg)
        return z

    lax.fori_loop(0, NK, bwd, 0)

    @pl.when(s == 0)
    def _():
        pltpu.make_async_copy(us.at[0, 0], ub.at[0], su.at[0]).wait()
    for i in range(4):
        tile_wait(hgb.at[i], shg.at[i])
    for i in range(2):
        tile_wait(hop.at[i], sop.at[i])
    pltpu.make_async_copy(hl.at[0], gl.at[0], sh0).wait()
    pltpu.make_async_copy(hl.at[0], gl.at[0], sg2).wait()
    for i in range(2):
        @pl.when(2 * c + i != e)
        def _():
            pltpu.make_async_copy(hl.at[i], gl.at[i], lh.at[i]).wait()
            pltpu.make_async_copy(hl.at[i], gl.at[i], lg.at[i]).wait()

    @pl.when(c == e // 2)
    def _():
        for i in range(2):
            wl_copy(i).wait_send()

    @pl.when(c != e // 2)
    def _():
        for i in range(2):
            wl_copy(i).wait_recv()


def _pipe(x, t, w1, w2, inv):
    hbm = pl.BlockSpec(memory_space=pl.ANY)
    dma = pltpu.SemaphoreType.DMA
    return pl.pallas_call(
        functools.partial(_pipe_kernel, inv),
        name="pipe",
        out_shape=(
            jax.ShapeDtypeStruct((2, TOK, D), BF16),
            jax.ShapeDtypeStruct((2, TOK, D), BF16),
            jax.ShapeDtypeStruct((D, FF), BF16),
            jax.ShapeDtypeStruct((FF, D), BF16),
            jax.ShapeDtypeStruct((2, NK, R, FF), BF16),
            jax.ShapeDtypeStruct((8, D), F32),
        ),
        in_specs=[hbm] * 4,
        out_specs=(hbm,) * 5 + (pl.BlockSpec(memory_space=pltpu.VMEM),),
        scratch_shapes=[
            pltpu.VMEM((2, D, FF), BF16),
            pltpu.VMEM((2, FF, D), BF16),
            pltpu.VMEM((NK, R, D), BF16),
            pltpu.VMEM((NK, R, D), BF16),
            pltpu.VMEM((2, R, FF), BF16),
            pltpu.VMEM((R, FF), BF16),
            pltpu.VMEM((4, R, D), BF16),
            pltpu.VMEM((2, R, D), BF16),
            pltpu.VMEM((R, D), BF16),
            dma((4,)), dma((NK,)), dma((NK,)), dma, dma((2,)), dma, dma,
            dma((4,)), dma((2,)), dma((2,)), dma((2,)), dma((2,)), dma((2,)),
        ],
        compiler_params=pltpu.CompilerParams(has_side_effects=True, vmem_limit_bytes=VMEM_LIMIT),
    )(x, t, w1, w2)


def _grad_kernel(hl, gl, w1, w2, wl1, wl2, o1, o2,
                 hres, gres, wb1, wb2, wt, p1, p2, r1, r2, f1, f2,
                 slh, slg, swb, sxs, sxr, ssl, sscw, ssccw, rab, rc, rd, sf):
    d = lax.axis_index('dp')
    s = lax.axis_index('pp')
    c = s % 2
    xx = s // 2
    t = d // 2
    j = d % 2
    zz = d // 2
    yy = d % 2
    nxt = 2 * yy + 1 - zz
    prv = 2 * (1 - yy) + zz
    tgt = 2 * xx + t
    partner = 2 * xx + 1 - c

    def load(q):
        src = (q % 2, pl.ds(pl.multiple_of((q // 2) * TC, TC), TC))
        dst = (pl.ds(pl.multiple_of(q * TC, TC), TC),)
        return (pltpu.make_async_copy(hl.at[src], hres.at[dst], slh.at[q]),
                pltpu.make_async_copy(gl.at[src], gres.at[dst], slg.at[q]))

    def wload_start(b):
        sl = b % 2
        cs = pl.ds(pl.multiple_of(b * BC, BC), BC)

        @pl.when(c == t)
        def _():
            pltpu.make_async_copy(w1.at[j, :, cs], wb1.at[sl], swb.at[sl, 0]).start()
            pltpu.make_async_copy(w2.at[j, cs, :], wb2.at[sl], swb.at[sl, 1]).start()

        @pl.when(c != t)
        def _():
            pltpu.make_async_copy(wl1.at[:, cs], wb1.at[sl], swb.at[sl, 0]).start()
            pltpu.make_async_copy(wl2.at[cs, :], wb2.at[sl], swb.at[sl, 1]).start()

    def wload_wait(b):
        sl = b % 2
        pltpu.make_async_copy(wl1.at[:, pl.ds(0, BC)], wb1.at[sl], swb.at[sl, 0]).wait()
        pltpu.make_async_copy(wl2.at[pl.ds(0, BC), :], wb2.at[sl], swb.at[sl, 1]).wait()

    wload_start(0)
    for q in range(NQ):
        for cp in load(q):
            cp.start()

    mine = pl.ds(pl.multiple_of(c * HB, HB), HB)
    theirs = pl.ds(pl.multiple_of((1 - c) * HB, HB), HB)

    def exchange(b):
        sl = b % 2
        return [pltpu.make_async_remote_copy(p.at[sl, theirs, :], r.at[sl], sxs.at[sl, i], sxr.at[sl, i],
                                             device_id=(d, partner), device_id_type=MESH)
                for i, (p, r) in enumerate(((p1, r1), (p2, r2)))]

    def region(i, jj, b, half):
        cs = pl.ds(pl.multiple_of(b * BC + half * HB, HB), HB)
        return o1.at[jj, :, cs] if i == 0 else o2.at[jj, cs, :]

    def finish(b):
        sl = b % 2
        for cp in exchange(b):
            cp.wait()
        f1[b] = (p1[sl, mine, :] + r1[sl]).T
        f2[b] = p2[sl, mine, :] + r2[sl]
        for i, f in enumerate((f1, f2)):
            dst = region(i, j, b, c)
            pltpu.make_async_remote_copy(f.at[b], dst, sscw.at[i], rab.at[c, i, b],
                                         device_id=(nxt, tgt), device_id_type=MESH).start()
            pltpu.make_async_remote_copy(f.at[b], dst, ssccw.at[i], rab.at[1 - c, i, b],
                                         device_id=(prv, tgt), device_id_type=MESH).start()

            @pl.when(c == t)
            def _():
                pltpu.make_async_copy(f.at[b], dst, ssl.at[i]).start()

            @pl.when(c != t)
            def _():
                pltpu.make_async_remote_copy(f.at[b], dst, ssl.at[i], rd.at[i],
                                             device_id=(d, tgt), device_id_type=MESH).start()

    def block(b, z):
        sl = b % 2
        wload_wait(b)
        wt[...] = wb1[sl].T
        p1[sl] = jnp.zeros((BC, D), F32)
        p2[sl] = jnp.zeros((BC, D), F32)

        @pl.when(b < NB - 1)
        def _():
            wload_start(b + 1)

        def chunk(q, z2):
            @pl.when(b == 0)
            def _():
                for cp in load(q):
                    cp.wait()

            rs = pl.ds(pl.multiple_of(q * TC, TC), TC)
            ut = _dot_t(wt[...], hres[rs, :])
            qt = _dot_t(wb2[sl], gres[rs, :])
            th, hu, t2 = _act(ut.astype(BF16).astype(F32))
            a = (hu + hu * th).astype(BF16)
            ee = (_dgelu(th, hu, t2) * qt).astype(BF16)
            p1[sl] += _dot(ee, hres[rs, :])
            p2[sl] += _dot(a, gres[rs, :])

            @pl.when(jnp.logical_and(q == 0, b > 0))
            def _():
                finish(b - 1)
            return z2

        lax.fori_loop(0, NQ, chunk, 0)
        for cp in exchange(b):
            cp.start()
        return z

    lax.fori_loop(0, NB, block, 0)
    finish(NB - 1)

    cw = prv // 2 == c
    src_chip = jnp.where(cw, prv, nxt)
    half = jnp.where(cw, 0, 1)
    onward = jnp.where(cw, nxt, prv)

    def forward(b, z):
        for i in range(2):
            reg = region(i, src_chip % 2, b, half)
            cp = pltpu.make_async_remote_copy(reg, reg, sf.at[i], rab.at[0, i, b],
                                              device_id=(onward, s), device_id_type=MESH)
            cp.wait_recv()
            pltpu.make_async_remote_copy(reg, reg, sf.at[i], rc.at[half, i],
                                         device_id=(onward, s), device_id_type=MESH).start()
        return z

    lax.fori_loop(0, NB, forward, 0)

    def others(b, z):
        for i in range(2):
            reg = region(i, src_chip % 2, b, 1 - half)
            pltpu.make_async_remote_copy(reg, reg, sf.at[i], rab.at[1, i, b],
                                         device_id=(onward, s), device_id_type=MESH).wait_recv()
        return z

    lax.fori_loop(0, NB, others, 0)

    for i, f in enumerate((f1, f2)):
        big = o1.at[0, :, pl.ds(0, FF // 2)] if i == 0 else o2.at[0, pl.ds(0, FF // 2), :]
        for sem in (sscw, ssccw, ssl):
            pltpu.make_async_copy(big, big, sem.at[i]).wait()
        pltpu.make_async_copy(big, big, sf.at[i]).wait()

        @pl.when(c == t)
        def _():
            pltpu.make_async_copy(big, big, rd.at[i]).wait()

        @pl.when(c != t)
        def _():
            pltpu.make_async_copy(big, big, rc.at[0, i]).wait()
            pltpu.make_async_copy(big, big, rc.at[1, i]).wait()


def _grads(hl, gl, w1, w2, wl1, wl2):
    hbm = pl.BlockSpec(memory_space=pl.ANY)
    dma = pltpu.SemaphoreType.DMA
    return pl.pallas_call(
        _grad_kernel,
        name="grads",
        out_shape=(jax.ShapeDtypeStruct((2, D, FF), F32), jax.ShapeDtypeStruct((2, FF, D), F32)),
        in_specs=[hbm] * 6,
        out_specs=(hbm, hbm),
        scratch_shapes=[
            pltpu.VMEM((2 * TOK, D), BF16),
            pltpu.VMEM((2 * TOK, D), BF16),
            pltpu.VMEM((2, D, BC), BF16),
            pltpu.VMEM((2, BC, D), BF16),
            pltpu.VMEM((BC, D), BF16),
            pltpu.VMEM((2, BC, D), F32),
            pltpu.VMEM((2, BC, D), F32),
            pltpu.VMEM((2, HB, D), F32),
            pltpu.VMEM((2, HB, D), F32),
            pltpu.VMEM((NB, D, HB), F32),
            pltpu.VMEM((NB, HB, D), F32),
            dma((NQ,)), dma((NQ,)), dma((2, 2)), dma((2, 2)), dma((2, 2)),
            dma((2,)), dma((2,)), dma((2,)), dma((2, 2, NB)), dma((2, 2)), dma((2,)), dma((2,)),
        ],
        compiler_params=pltpu.CompilerParams(has_side_effects=True, vmem_limit_bytes=VMEM_LIMIT),
    )(hl, gl, w1, w2, wl1, wl2)


def solution(mesh):
    ndp = mesh.shape['dp']

    def body(x, t, w1, w2):
        nm, tok, d = x.shape
        inv = 1.0 / (nm * tok * ndp * d)
        hl, gl, wl1, wl2, _, lo = _pipe(x, t, w1[0], w2[0], inv)
        dw1, dw2 = _grads(hl, gl, w1[0], w2[0], wl1, wl2)
        loss = lax.psum(jnp.sum(lo) * (0.5 * inv), ('dp', 'pp'))
        return dw1[None], dw2[None], loss

    return jax.shard_map(body, mesh=mesh,
                         in_specs=(P(None, 'dp', None), P(None, 'dp', None), P('pp'), P('pp')),
                         out_specs=(P('pp'), P('pp'), P()), check_vma=False)
```

```python
import functools
import math

import jax
import jax.numpy as jnp
from jax import lax
from jax.experimental import pallas as pl
from jax.experimental.pallas import tpu as pltpu
from jax.sharding import PartitionSpec as P

MESH = pl.DeviceIdType.MESH
F32 = jnp.float32
BF16 = jnp.bfloat16
VMEM_LIMIT = 67_043_328
C0 = math.sqrt(2.0 / math.pi)
C1 = 0.044715

D = 1024
FF = 4096
R = 256
NK = 16
FC = 256
NF = FF // FC
ND = D // FC
LAG, TAIL = 2, 2
TOK = R * NK

BC = 256
NB = FF // BC
HB = BC // 2
NS = 2
TC = 1024
NQ = 2 * TOK // TC
SPG = TC // R

NT = (((1,), (1,)), ((), ()))


def _dot(a, b):
    return jnp.dot(a, b, preferred_element_type=F32)


def _dot_t(a, b):
    return lax.dot_general(a, b, NT, preferred_element_type=F32)


def _t(i):
    return slice(i * FC, (i + 1) * FC)


def _sum(parts):
    return functools.reduce(lambda a, b: a + b, parts)


def _act(u):
    t2 = u * u
    th = jnp.tanh(u * (C0 + (C0 * C1) * t2))
    return th, 0.5 * u, t2


def _gelu(u):
    th, hu, _ = _act(u)
    return hu + hu * th


def _dgelu(th, hu, t2):
    return (0.5 + 0.5 * th) + (hu * (1.0 - th * th)) * (C0 + (3.0 * C0 * C1) * t2)


def _chain(up, mid, down, lag, tail):
    acc = [None] * ND
    act = {}

    def add(f, n):
        part = down(f, n, act[f])
        acc[n] = part if acc[n] is None else acc[n] + part

    for f in range(NF + lag):
        if f < NF:
            act[f] = mid(f, up(f))
        if lag <= f < NF + lag - tail:
            for n in range(ND):
                add(f - lag, n)
    for n in range(ND):
        for f in range(NF - tail, NF):
            add(f, n)
    return acc


def _kernel(inv, x, t, w1, w2, o1, o2, oloss, hl, gl, wl1, wl2, us,
            W1, W2, hin, gin, hgb, r1, r2, lo, lt,
            sw, sx, sg, su, sh0, sg2, shg, sop, lh, lg, swl, rwl,
            sld, swb, sxs, sxr, ssl, sscw, ssccw, rab, rc, rd, sf, slt, rlt):
    e = lax.axis_index('dp')
    s = lax.axis_index('pp')
    c = s % 2
    xx = s // 2
    owner = e // 2
    tcore = 2 * xx + owner
    partner = 2 * xx + 1 - c
    first = s == 0
    last = s == 3


    def wcopy(j, i):
        if i == 0:
            return pltpu.make_async_copy(w1.at[j], W1.at[j], sw.at[2 * j])
        return pltpu.make_async_copy(w2.at[j], W2.at[j], sw.at[2 * j + 1])

    for j in range(2):
        for i in range(2):
            wcopy(j, i).start()

    def micro(arr, k):
        return arr.at[k // 2, pl.ds(pl.multiple_of((k % 2) * R, R), R)]

    def xcopy(k):
        return pltpu.make_async_copy(micro(x, k), hin.at[k], sx.at[k])

    def tcopy(k):
        return pltpu.make_async_copy(micro(t, k), gin.at[k], sg.at[k])

    @pl.when(first)
    def _():
        lax.fori_loop(0, NK, lambda k, z: (xcopy(k).start(), z)[1], 0)

    @pl.when(last)
    def _():
        lax.fori_loop(0, NK, lambda k, z: (tcopy(k).start(), z)[1], 0)

    def wl_copy(i):
        src, dst = ((w1, wl1), (w2, wl2))[i]
        return pltpu.make_async_remote_copy(src.at[e % 2], dst, swl.at[i], rwl.at[i],
                                            device_id=(e, partner), device_id_type=MESH)

    @pl.when(c == owner)
    def _():
        for i in range(2):
            wl_copy(i).start()

    lo[...] = jnp.zeros_like(lo)


    def rows(k):
        return pl.ds(pl.multiple_of(k * R, R), R)

    def ship(src, dst, k, j, sem, land):
        d = 2 * c + j

        @pl.when(d == e)
        def _():
            pltpu.make_async_copy(src, dst.at[e % 2, rows(k)], sem).start()

        @pl.when(d != e)
        def _():
            pltpu.make_async_remote_copy(src, dst.at[e % 2, rows(k)], sem, land.at[e % 2, k // SPG],
                                         device_id=(d, tcore), device_id_type=MESH).start()

    def tile_wait(buf, sem):
        pltpu.make_async_copy(buf, hl.at[0, pl.ds(0, R)], sem).wait()

    def pipeline(ub, hop):
        def store_wait(p, j):
            pltpu.make_async_copy(ub.at[p, j], us.at[j, 0], su.at[p, j]).wait()

        def fwd(k, z):
            h4 = k % 4
            h2 = k % 2
            pltpu.make_async_copy(hl.at[0, pl.ds(0, R)], hin.at[k], sx.at[k]).wait()

            @pl.when(k == 0)
            def _():
                for j in range(2):
                    wcopy(j, 0).wait()
                    wcopy(j, 1).wait()

            @pl.when(k >= 2)
            def _():
                store_wait(h2, 0)
                store_wait(h2, 1)

            @pl.when(k >= 4)
            def _():
                tile_wait(hgb.at[h4], shg.at[h4])

            @pl.when(jnp.logical_and(k >= 2, s < 3))
            def _():
                tile_wait(hop.at[h2], sop.at[h2])
            ship(hin.at[k], hl, k, 0, sh0, lh)

            def layer(h, j, dst):
                def up(f):
                    return _sum(_dot(h[i], W1[j, _t(i), _t(f)]) for i in range(ND))

                def mid(f, u):
                    u = u.astype(BF16)
                    ub[h2, j, :, _t(f)] = u
                    return _gelu(u.astype(F32)).astype(BF16)

                def down(f, n, a):
                    return _dot(a, W2[j, _t(f), _t(n)])

                out = []
                for n, v in enumerate(_chain(up, mid, down, LAG, TAIL)):
                    out.append((h[n].astype(F32) + v).astype(BF16))
                    dst[:, _t(n)] = out[n]
                return out

            h1 = layer([hin[k, :, _t(n)] for n in range(ND)], 0, hgb.at[h4])
            layer(h1, 1, hop.at[h2])

            @pl.when(s < 3)
            def _():
                pltpu.make_async_remote_copy(hop.at[h2], hin.at[k], sop.at[h2], sx.at[k],
                                             device_id=(e, s + 1), device_id_type=MESH).start()
            for j in range(2):
                pltpu.make_async_copy(ub.at[h2, j], us.at[j, k], su.at[h2, j]).start()
            ship(hgb.at[h4], hl, k, 1, shg.at[h4], lh)

            @pl.when(last)
            def _():
                tcopy(k).wait()
                r = hop[h2].astype(F32) - gin[k].astype(F32)
                lo[...] += jnp.sum((r * r).reshape(R // 8, 8, D), axis=0)
                gin[k] = (r * inv).astype(BF16)
            return z

        lax.fori_loop(0, NK, fwd, 0)

        def uload(k, j):
            return pltpu.make_async_copy(us.at[j, k], ub.at[k % 2, j], su.at[k % 2, j])

        for k in range(2):
            for j in range(2):
                store_wait(k, j)
                uload(k, j).start()

        def bwd(k, z):
            h4 = k % 4
            h2 = k % 2

            @pl.when(s < 3)
            def _():
                pltpu.make_async_copy(hl.at[0, pl.ds(0, R)], gin.at[k], sg.at[k]).wait()
            uload(k, 0).wait()
            uload(k, 1).wait()
            tile_wait(hgb.at[h4], shg.at[h4])

            @pl.when(jnp.where(s == 0, k < 2, jnp.logical_or(k >= 2, s < 3)))
            def _():
                tile_wait(hop.at[h2], sop.at[h2])
            ship(gin.at[k], gl, k, 1, sg2, lg)

            def layer(g, j, dst):
                def up(f):
                    return _sum(_dot_t(g[i], W2[j, _t(f), _t(i)]) for i in range(ND))

                def mid(f, q):
                    th, hu, t2 = _act(ub[h2, j, :, _t(f)].astype(F32))
                    return (_dgelu(th, hu, t2) * q).astype(BF16)

                def down(f, n, ee):
                    return _dot_t(ee, W1[j, _t(n), _t(f)])

                out = []
                for n, v in enumerate(_chain(up, mid, down, LAG, TAIL)):
                    out.append((g[n].astype(F32) + v).astype(BF16))
                    dst[:, _t(n)] = out[n]
                return out

            def g2():
                return [gin[k, :, _t(n)] for n in range(ND)]

            @pl.when(s == 0)
            def _():
                layer(g2(), 1, hgb.at[h4])

            @pl.when(s > 0)
            def _():
                layer(layer(g2(), 1, hgb.at[h4]), 0, hop.at[h2])
                pltpu.make_async_remote_copy(hop.at[h2], gin.at[k], sop.at[h2], sg.at[k],
                                             device_id=(e, s - 1), device_id_type=MESH).start()
            ship(hgb.at[h4], gl, k, 0, shg.at[h4], lg)

            @pl.when(k < NK - 2)
            def _():
                uload(k + 2, 0).start()
                uload(k + 2, 1).start()
            return z

        lax.fori_loop(0, NK, bwd, 0)

        @pl.when(s > 0)
        def _():
            for i in range(2):
                tile_wait(hop.at[i], sop.at[i])

    pl.run_scoped(pipeline, pltpu.VMEM((2, 2, R, FF), BF16), pltpu.VMEM((2, R, D), BF16))


    jj = e % 2
    zz = e // 2
    yy = e % 2
    nxt = 2 * yy + 1 - zz
    prv = 2 * (1 - yy) + zz

    def shipped(j):
        if j == 0:
            pltpu.make_async_copy(hl.at[0], gl.at[0], sh0).wait()
            for i in range(4):
                tile_wait(hgb.at[i], shg.at[i])
        else:
            pltpu.make_async_copy(hl.at[0], gl.at[0], sg2).wait()

    for j in range(2):
        @pl.when(2 * c + j == e)
        def _():
            shipped(j)

    @pl.when(c != owner)
    def _():
        for i in range(2):
            wl_copy(i).wait_recv()

    @pl.when(last)
    def _():
        v = lo[:, :128]
        for i in range(1, D // 128):
            v = v + lo[:, i * 128:(i + 1) * 128]
        lt[e] = v

    def loss_copy(i):
        to = (4 * e + s + i) % 16
        return pltpu.make_async_remote_copy(lt.at[e], lt.at[e], slt.at[i], rlt.at[e],
                                            device_id=(to // 4, to % 4), device_id_type=MESH)

    def hview(q):
        return W2.at[q // 4, pl.ds(pl.multiple_of((q % 4) * TC, TC), TC), :]

    def gview(q):
        return W1.at[q // 4, :, pl.ds(pl.multiple_of((q % 4) * D, D), D)]

    def landed(q):
        sl = q % 2

        @pl.when(2 * c + sl != e)
        def _():
            part = hl.at[0, pl.ds(0, TC)]
            pltpu.make_async_copy(part, part, lh.at[sl, q // 2]).wait()
            pltpu.make_async_copy(part, part, lg.at[sl, q // 2]).wait()

    def load(q):
        src = (q % 2, pl.ds(pl.multiple_of((q // 2) * TC, TC), TC))
        return (pltpu.make_async_copy(hl.at[src], hview(q), sld.at[0, q]),
                pltpu.make_async_copy(gl.at[src], gview(q), sld.at[1, q]))

    def region(i, j, b, half):
        cs = pl.ds(pl.multiple_of(b * BC + half * HB, HB), HB)
        return o1.at[j, :, cs] if i == 0 else o2.at[j, cs, :]

    def grads(wb1, wb2, wt, p1, p2, f1, f2):
        def wload_start(b):
            sl = b % 2
            cs = pl.ds(pl.multiple_of(b * BC, BC), BC)

            @pl.when(c == owner)
            def _():
                pltpu.make_async_copy(w1.at[jj, :, cs], wb1.at[sl], swb.at[sl, 0]).start()
                pltpu.make_async_copy(w2.at[jj, cs, :], wb2.at[sl], swb.at[sl, 1]).start()

            @pl.when(c != owner)
            def _():
                pltpu.make_async_copy(wl1.at[:, cs], wb1.at[sl], swb.at[sl, 0]).start()
                pltpu.make_async_copy(wl2.at[cs, :], wb2.at[sl], swb.at[sl, 1]).start()

        def wload_wait(b):
            sl = b % 2
            pltpu.make_async_copy(wl1.at[:, pl.ds(0, BC)], wb1.at[sl], swb.at[sl, 0]).wait()
            pltpu.make_async_copy(wl2.at[pl.ds(0, BC), :], wb2.at[sl], swb.at[sl, 1]).wait()

        def start_load(q):
            landed(q)
            for cp in load(q):
                cp.start()

        wload_start(0)
        start_load(0)

        mine = pl.ds(pl.multiple_of(c * HB, HB), HB)
        theirs = pl.ds(pl.multiple_of((1 - c) * HB, HB), HB)

        def exchange(b):
            sl = b % 2
            return [pltpu.make_async_remote_copy(p.at[sl, theirs, :], r.at[sl], sxs.at[sl, i], sxr.at[sl, i],
                                                 device_id=(e, partner), device_id_type=MESH)
                    for i, (p, r) in enumerate(((p1, r1), (p2, r2)))]

        def sent(b):
            for i, f in enumerate((f1, f2)):
                for sem in (sscw, ssccw, ssl):
                    pltpu.make_async_copy(f.at[b % NS], region(i, 0, 0, 0), sem.at[i, b % NS]).wait()

        def finish(b):
            sl = b % 2
            fs = b % NS
            for cp in exchange(b):
                cp.wait()

            @pl.when(b >= NS)
            def _():
                sent(b)
            f1[fs] = (p1[sl, mine, :] + r1[sl]).T
            f2[fs] = p2[sl, mine, :] + r2[sl]
            for i, f in enumerate((f1, f2)):
                dst = region(i, jj, b, c)
                pltpu.make_async_remote_copy(f.at[fs], dst, sscw.at[i, fs], rab.at[c, i, b],
                                             device_id=(nxt, tcore), device_id_type=MESH).start()
                pltpu.make_async_remote_copy(f.at[fs], dst, ssccw.at[i, fs], rab.at[1 - c, i, b],
                                             device_id=(prv, tcore), device_id_type=MESH).start()

                @pl.when(c == owner)
                def _():
                    pltpu.make_async_copy(f.at[fs], dst, ssl.at[i, fs]).start()

                @pl.when(c != owner)
                def _():
                    pltpu.make_async_remote_copy(f.at[fs], dst, ssl.at[i, fs], rd.at[i],
                                                 device_id=(e, tcore), device_id_type=MESH).start()

        def block(b, z):
            sl = b % 2
            wload_wait(b)
            wt[...] = wb1[sl].T
            p1[sl] = jnp.zeros((BC, D), F32)
            p2[sl] = jnp.zeros((BC, D), F32)

            @pl.when(b < NB - 1)
            def _():
                wload_start(b + 1)

            def chunk(q, z2):
                @pl.when(b == 0)
                def _():
                    @pl.when(q < NQ - 3)
                    def _():
                        start_load(q + 1)
                    for cp in load(q):
                        cp.wait()

                hq = hview(q)
                gq = gview(q)
                es, acts = [], []
                for i in range(TC // FC):
                    ut = _dot_t(wt[...], hq[_t(i), :])
                    qt = _dot_t(wb2[sl], gq[_t(i), :])
                    th, hu, t2 = _act(ut.astype(BF16).astype(F32))
                    acts.append((hu + hu * th).astype(BF16))
                    es.append((_dgelu(th, hu, t2) * qt).astype(BF16))
                for n in range(ND):
                    p1[sl, :, _t(n)] += _sum(_dot(es[i], hq[_t(i), _t(n)]) for i in range(TC // FC))
                    p2[sl, :, _t(n)] += _sum(_dot(acts[i], gq[_t(i), _t(n)]) for i in range(TC // FC))

                @pl.when(jnp.logical_and(b == 0, q == NQ - 3))
                def _():
                    start_load(NQ - 2)
                    start_load(NQ - 1)

                @pl.when(jnp.logical_and(q == 0, b > 0))
                def _():
                    finish(b - 1)
                return z2

            lax.fori_loop(0, NQ, chunk, 0)
            for cp in exchange(b):
                cp.start()
            return z

        lax.fori_loop(0, 1, block, 0)

        @pl.when(last)
        def _():
            for i in range(1, 16):
                loss_copy(i).start()

        lax.fori_loop(1, NB, block, 0)
        finish(NB - 1)
        for b in range(NB - NS, NB):
            sent(b)

    pl.run_scoped(grads, pltpu.VMEM((2, D, BC), BF16), pltpu.VMEM((2, BC, D), BF16), pltpu.VMEM((BC, D), BF16),
                  pltpu.VMEM((2, BC, D), F32), pltpu.VMEM((2, BC, D), F32),
                  pltpu.VMEM((NS, D, HB), F32), pltpu.VMEM((NS, HB, D), F32))

    cw = prv // 2 == c
    src_chip = jnp.where(cw, prv, nxt)
    half = jnp.where(cw, 0, 1)
    onward = jnp.where(cw, nxt, prv)

    def forward(b, z):
        for i in range(2):
            reg = region(i, src_chip % 2, b, half)
            pltpu.make_async_remote_copy(reg, reg, sf.at[i], rab.at[0, i, b],
                                         device_id=(onward, s), device_id_type=MESH).wait_recv()
            pltpu.make_async_remote_copy(reg, reg, sf.at[i], rc.at[half, i],
                                         device_id=(onward, s), device_id_type=MESH).start()
        return z

    lax.fori_loop(0, NB, forward, 0)

    def others(b, z):
        for i in range(2):
            reg = region(i, src_chip % 2, b, 1 - half)
            pltpu.make_async_remote_copy(reg, reg, sf.at[i], rab.at[1, i, b],
                                         device_id=(onward, s), device_id_type=MESH).wait_recv()
        return z

    lax.fori_loop(0, NB, others, 0)


    for i in range(2):
        big = o1.at[0, :, pl.ds(0, FF // 2)] if i == 0 else o2.at[0, pl.ds(0, FF // 2), :]
        pltpu.make_async_copy(big, big, sf.at[i]).wait()

        @pl.when(c == owner)
        def _():
            pltpu.make_async_copy(big, big, rd.at[i]).wait()

        @pl.when(c != owner)
        def _():
            pltpu.make_async_copy(big, big, rc.at[0, i]).wait()
            pltpu.make_async_copy(big, big, rc.at[1, i]).wait()

    for j in range(2):
        @pl.when(2 * c + j != e)
        def _():
            shipped(j)

    @pl.when(c == owner)
    def _():
        for i in range(2):
            wl_copy(i).wait_send()

    @pl.when(last)
    def _():
        for i in range(1, 16):
            loss_copy(i).wait_send()

    for i in range(4):
        @pl.when(jnp.logical_not(jnp.logical_and(last, e == i)))
        def _():
            pltpu.make_async_remote_copy(lt.at[i], lt.at[i], slt.at[0], rlt.at[i],
                                         device_id=(e, s), device_id_type=MESH).wait_recv()
    oloss[0, 0] = jnp.sum((lt[0] + lt[1]) + (lt[2] + lt[3])) * (0.5 * inv)


def _call(x, t, w1, w2, inv):
    hbm = pl.BlockSpec(memory_space=pl.ANY)
    dma = pltpu.SemaphoreType.DMA
    vmem = pltpu.VMEM
    out = pl.pallas_call(
        functools.partial(_kernel, inv),
        name="train_step",
        out_shape=(
            jax.ShapeDtypeStruct((2, D, FF), F32),
            jax.ShapeDtypeStruct((2, FF, D), F32),
            jax.ShapeDtypeStruct((1, 1), F32),
            jax.ShapeDtypeStruct((2, TOK, D), BF16),
            jax.ShapeDtypeStruct((2, TOK, D), BF16),
            jax.ShapeDtypeStruct((D, FF), BF16),
            jax.ShapeDtypeStruct((FF, D), BF16),
            jax.ShapeDtypeStruct((2, NK, R, FF), BF16),
        ),
        in_specs=[hbm] * 4,
        out_specs=(hbm, hbm, pl.BlockSpec(memory_space=pltpu.SMEM)) + (hbm,) * 5,
        scratch_shapes=[
            vmem((2, D, FF), BF16), vmem((2, FF, D), BF16),
            vmem((NK, R, D), BF16), vmem((NK, R, D), BF16), vmem((4, R, D), BF16),
            vmem((2, HB, D), F32), vmem((2, HB, D), F32),
            vmem((8, D), F32), vmem((4, 8, 128), F32),
            dma((4,)), dma((NK,)), dma((NK,)), dma((2, 2)), dma, dma,
            dma((4,)), dma((2,)), dma((2, NK // SPG)), dma((2, NK // SPG)), dma((2,)), dma((2,)),
            dma((2, NQ)), dma((2, 2)), dma((2, 2)), dma((2, 2)),
            dma((2, NS)), dma((2, NS)), dma((2, NS)), dma((2, 2, NB)), dma((2, 2)), dma((2,)), dma((2,)),
            dma((16,)), dma((4,)),
        ],
        compiler_params=pltpu.CompilerParams(has_side_effects=True, vmem_limit_bytes=VMEM_LIMIT),
    )(x, t, w1, w2)
    return out[:3]


def solution(mesh):
    ndp = mesh.shape['dp']

    def body(x, t, w1, w2):
        nm, tok, d = x.shape
        dw1, dw2, loss = _call(x, t, w1[0], w2[0], 1.0 / (nm * tok * ndp * d))
        return dw1[None], dw2[None], loss[0, 0]

    return jax.shard_map(body, mesh=mesh,
                         in_specs=(P(None, 'dp', None), P(None, 'dp', None), P('pp'), P('pp')),
                         out_specs=(P('pp'), P('pp'), P()), check_vma=False)
```

```python
import functools
import math

import jax
import jax.numpy as jnp
from jax import lax
from jax.experimental import pallas as pl
from jax.experimental.pallas import tpu as pltpu
from jax.sharding import PartitionSpec as P

MESH = pl.DeviceIdType.MESH
F32 = jnp.float32
BF16 = jnp.bfloat16
VMEM_LIMIT = 67_043_328
C0 = math.sqrt(2.0 / math.pi)
C1 = 0.044715

D = 1024
FF = 4096
R = 256
NK = 16
FC = 256
NF = FF // FC
ND = D // FC
LAG, TAIL = 2, 2
TOK = R * NK

BC = 256
NB = FF // BC
HB = BC // 2
NS = 2
NR = 6
EARLY = 6
NL = 4
TP = 1024
NP = 2 * TOK // TP
SPG = TP // R
PQ = 2
NQ = NP // PQ
GT = 2

NT = (((1,), (1,)), ((), ()))


def _dot(a, b):
    return jnp.dot(a, b, preferred_element_type=F32)


def _dot_t(a, b):
    return lax.dot_general(a, b, NT, preferred_element_type=F32)


def _t(i):
    return slice(i * FC, (i + 1) * FC)


def _sum(parts):
    return functools.reduce(lambda a, b: a + b, parts)


def _act(u):
    t2 = u * u
    th = jnp.tanh(u * (C0 + (C0 * C1) * t2))
    return th, 0.5 * u, t2


def _gelu(u):
    th, hu, _ = _act(u)
    return hu + hu * th


def _dgelu(th, hu, t2):
    return (0.5 + 0.5 * th) + (hu * (1.0 - th * th)) * (C0 + (3.0 * C0 * C1) * t2)


def _chain(up, mid, down, lag, tail):
    acc = [None] * ND
    act = {}

    def add(f, n):
        part = down(f, n, act[f])
        acc[n] = part if acc[n] is None else acc[n] + part

    for f in range(NF + lag):
        if f < NF:
            act[f] = mid(f, up(f))
        if lag <= f < NF + lag - tail:
            for n in range(ND):
                add(f - lag, n)
    for n in range(ND):
        for f in range(NF - tail, NF):
            add(f, n)
    return acc


def _kernel(inv, x, t, w1, w2, fw1, fw2, fw3, ot1, ot2, sf1, sf2, oloss, hl, gl, wl1, wl2, us,
            W1, W2, hin, gin, hgb, r1, r2, lo, lt,
            sw, sx, sg, su, sh0, sg2, shg, sop, lh, lg, swl, rwl,
            sld, swb, sxs, sxr, ssl, sscw, ssccw, rn, rd, slt, rlt, free):
    e = lax.axis_index('dp')
    s = lax.axis_index('pp')
    c = s % 2
    xx = s // 2
    owner = e // 2
    tcore = 2 * xx + owner
    partner = 2 * xx + 1 - c
    first = s == 0
    last = s == 3


    def wcopy(j, i):
        if i == 0:
            return pltpu.make_async_copy(w1.at[j], W1.at[j], sw.at[2 * j])
        return pltpu.make_async_copy(w2.at[j], W2.at[j], sw.at[2 * j + 1])

    for j in range(2):
        for i in range(2):
            wcopy(j, i).start()

    def micro(arr, k):
        return arr.at[k // 2, pl.ds(pl.multiple_of((k % 2) * R, R), R)]

    def xcopy(k):
        return pltpu.make_async_copy(micro(x, k), hin.at[k], sx.at[k])

    def tcopy(k):
        return pltpu.make_async_copy(micro(t, k), gin.at[k], sg.at[k])

    @pl.when(first)
    def _():
        lax.fori_loop(0, NK, lambda k, z: (xcopy(k).start(), z)[1], 0)

    @pl.when(last)
    def _():
        lax.fori_loop(0, NK, lambda k, z: (tcopy(k).start(), z)[1], 0)

    def wl_copy(i):
        src, dst = ((w1, wl1), (w2, wl2))[i]
        return pltpu.make_async_remote_copy(src.at[e % 2], dst, swl.at[i], rwl.at[i],
                                            device_id=(e, partner), device_id_type=MESH)

    @pl.when(c == owner)
    def _():
        for i in range(2):
            wl_copy(i).start()

    lo[...] = jnp.zeros_like(lo)


    def rows(k):
        return pl.ds(pl.multiple_of(k * R, R), R)

    def ship(src, dst, k, j, sem, land):
        d = 2 * c + j

        @pl.when(d == e)
        def _():
            pltpu.make_async_copy(src, dst.at[e % 2, rows(k)], sem).start()

        @pl.when(d != e)
        def _():
            pltpu.make_async_remote_copy(src, dst.at[e % 2, rows(k)], sem, land.at[e % 2, k // SPG],
                                         device_id=(d, tcore), device_id_type=MESH).start()

    def tile_wait(buf, sem):
        pltpu.make_async_copy(buf, hl.at[0, pl.ds(0, R)], sem).wait()

    ahead = jnp.where(last, EARLY, NK)

    def pipeline(ub, hop):
        def ustore(p, k, j):
            return pltpu.make_async_copy(ub.at[p, j], us.at[j, k], su.at[p, j])

        def uload(p, k):
            for j in range(2):
                pltpu.make_async_copy(us.at[j, k], ub.at[p, j], su.at[p, j]).start()

        def uwait(p):
            for j in range(2):
                pltpu.make_async_copy(us.at[j, 0], ub.at[p, j], su.at[p, j]).wait()

        def fwd(k):
            n = jnp.where(k < ahead, k, 2 * k - ahead)
            h4 = n % NR
            h2 = jnp.where(last, 0, k % 2)
            p = jnp.where(k < ahead, (ahead - 1 - k) % 2, 0)
            pltpu.make_async_copy(hl.at[0, pl.ds(0, R)], hin.at[k], sx.at[k]).wait()

            @pl.when(k == 0)
            def _():
                for j in range(2):
                    wcopy(j, 0).wait()
                    wcopy(j, 1).wait()

            @pl.when(k >= 2)
            def _():
                uwait(p)

            @pl.when(n >= NR)
            def _():
                tile_wait(hgb.at[h4], shg.at[h4])

            @pl.when(jnp.logical_and(k >= 2, s < 3))
            def _():
                tile_wait(hop.at[h2], sop.at[h2])
            ship(hin.at[k], hl, k, 0, sh0, lh)

            def layer(h, j, dst):
                def up(f):
                    return _sum(_dot(h[i], W1[j, _t(i), _t(f)]) for i in range(ND))

                def mid(f, u):
                    u = u.astype(BF16)
                    ub[p, j, :, _t(f)] = u
                    return _gelu(u.astype(F32)).astype(BF16)

                def down(f, n, a):
                    return _dot(a, W2[j, _t(f), _t(n)])

                out = []
                for n, v in enumerate(_chain(up, mid, down, LAG, TAIL)):
                    out.append((h[n].astype(F32) + v).astype(BF16))
                    dst[:, _t(n)] = out[n]
                return out

            h1 = layer([hin[k, :, _t(n)] for n in range(ND)], 0, hgb.at[h4])
            layer(h1, 1, hop.at[h2])

            @pl.when(s < 3)
            def _():
                pltpu.make_async_remote_copy(hop.at[h2], hin.at[k], sop.at[h2], sx.at[k],
                                             device_id=(e, s + 1), device_id_type=MESH).start()
            for j in range(2):
                ustore(p, k, j).start()
            ship(hgb.at[h4], hl, k, 1, shg.at[h4], lh)

            @pl.when(last)
            def _():
                tcopy(k).wait()
                r = hop[h2].astype(F32) - gin[k].astype(F32)
                lo[...] += jnp.sum((r * r).reshape(R // 8, 8, D), axis=0)
                gin[k] = (r * inv).astype(BF16)

        def bwd(i):
            k = i - ahead
            n = jnp.where(i < NK, 2 * i - ahead + 1, NK - ahead + i)
            h4 = n % NR
            h2 = jnp.where(last, 1, k % 2)
            p = jnp.where(i < NK, 1, (i - NK + 1) % 2)

            @pl.when(s < 3)
            def _():
                pltpu.make_async_copy(hl.at[0, pl.ds(0, R)], gin.at[k], sg.at[k]).wait()
            uwait(p)

            @pl.when(n >= NR)
            def _():
                tile_wait(hgb.at[h4], shg.at[h4])

            @pl.when(jnp.where(s == 0, k < 2, jnp.where(last, k >= 1, k >= 0)))
            def _():
                tile_wait(hop.at[h2], sop.at[h2])
            ship(gin.at[k], gl, k, 1, sg2, lg)

            def layer(g, j, dst):
                def up(f):
                    return _sum(_dot_t(g[i], W2[j, _t(f), _t(i)]) for i in range(ND))

                def mid(f, q):
                    th, hu, t2 = _act(ub[p, j, :, _t(f)].astype(F32))
                    return (_dgelu(th, hu, t2) * q).astype(BF16)

                def down(f, n, ee):
                    return _dot_t(ee, W1[j, _t(n), _t(f)])

                out = []
                for n, v in enumerate(_chain(up, mid, down, LAG, TAIL)):
                    out.append((g[n].astype(F32) + v).astype(BF16))
                    dst[:, _t(n)] = out[n]
                return out

            def g2():
                return [gin[k, :, _t(n)] for n in range(ND)]

            @pl.when(s == 0)
            def _():
                layer(g2(), 1, hgb.at[h4])

            @pl.when(s > 0)
            def _():
                layer(layer(g2(), 1, hgb.at[h4]), 0, hop.at[h2])
                pltpu.make_async_remote_copy(hop.at[h2], gin.at[k], sop.at[h2], sg.at[k],
                                             device_id=(e, s - 1), device_id_type=MESH).start()
            ship(hgb.at[h4], gl, k, 0, shg.at[h4], lg)

            @pl.when(jnp.logical_and(i >= NK, k < NK - 2))
            def _():
                uload(p, k + 2)

        def step(i, z):
            @pl.when(i < NK)
            def _():
                fwd(i)

            @pl.when(jnp.logical_and(i >= ahead, i < NK + ahead))
            def _():
                bwd(i)

            @pl.when(i == ahead - 1)
            def _():
                uwait(1)

            @pl.when(jnp.logical_and(i >= ahead - 1, i < NK))
            def _():
                uload(1, i + 1 - ahead)

            @pl.when(i == NK - 1)
            def _():
                uwait(0)
                uload(0, NK + 1 - ahead)
            return z

        lax.fori_loop(0, 2 * NK, step, 0)

        @pl.when(last)
        def _():
            tile_wait(hop.at[1], sop.at[1])

        @pl.when(jnp.logical_and(s > 0, s < 3))
        def _():
            for i in range(2):
                tile_wait(hop.at[i], sop.at[i])

    pl.run_scoped(pipeline, pltpu.VMEM((2, 2, R, FF), BF16), pltpu.VMEM((2, R, D), BF16))


    jj = e % 2
    zz = e // 2
    yy = e % 2
    nxt = 2 * yy + 1 - zz
    prv = 2 * (1 - yy) + zz

    def shipped(j):
        if j == 0:
            pltpu.make_async_copy(hl.at[0], gl.at[0], sh0).wait()
            for i in range(NR):
                tile_wait(hgb.at[i], shg.at[i])
        else:
            pltpu.make_async_copy(hl.at[0], gl.at[0], sg2).wait()

    for j in range(2):
        @pl.when(2 * c + j == e)
        def _():
            shipped(j)

    @pl.when(c != owner)
    def _():
        for i in range(2):
            wl_copy(i).wait_recv()

    @pl.when(last)
    def _():
        v = lo[:, :128]
        for i in range(1, D // 128):
            v = v + lo[:, i * 128:(i + 1) * 128]
        lt[e] = v

    def loss_copy(i):
        to = (4 * e + s + i) % 16
        return pltpu.make_async_remote_copy(lt.at[e], lt.at[e], slt.at[i], rlt.at[e],
                                            device_id=(to // 4, to % 4), device_id_type=MESH)

    def hview(q):
        return W2.at[q // 4, pl.ds(pl.multiple_of((q % 4) * TP, TP), TP), :]

    def gview(q):
        return W1.at[q // 4, :, pl.ds(pl.multiple_of((q % 4) * D, D), D)]

    def landed(q):
        sl = q % 2

        @pl.when(2 * c + sl != e)
        def _():
            part = hl.at[0, pl.ds(0, TP)]
            pltpu.make_async_copy(part, part, lh.at[sl, q // 2]).wait()
            pltpu.make_async_copy(part, part, lg.at[sl, q // 2]).wait()

    def load(q):
        src = (q % 2, pl.ds(pl.multiple_of((q // 2) * TP, TP), TP))
        return (pltpu.make_async_copy(hl.at[src], hview(q), sld.at[0, q]),
                pltpu.make_async_copy(gl.at[src], gview(q), sld.at[1, q]))

    def grads(wb1, wb2, wt, p1, p2, f1, f2):
        def wload(b, i):
            cs = pl.ds(pl.multiple_of(b * BC, BC), BC)
            own, got, buf = ((w1.at[jj, :, cs], wl1.at[:, cs], wb1), (w2.at[jj, cs, :], wl2.at[cs, :], wb2))[i]

            @pl.when(c == owner)
            def _():
                pltpu.make_async_copy(own, buf.at[b % 2], swb.at[b % 2, i]).start()

            @pl.when(c != owner)
            def _():
                pltpu.make_async_copy(got, buf.at[b % 2], swb.at[b % 2, i]).start()

        def wwait(b, i):
            got, buf = ((wl1.at[:, pl.ds(0, BC)], wb1), (wl2.at[pl.ds(0, BC), :], wb2))[i]
            pltpu.make_async_copy(got, buf.at[b % 2], swb.at[b % 2, i]).wait()

        def start_load(q):
            landed(q)
            for cp in load(q):
                cp.start()

        wload(0, 0)
        wload(0, 1)
        wload(1, 0)
        for q in range(2 * PQ):
            start_load(q)
        wwait(0, 0)
        wt[0] = wb1[0].T

        @pl.when(last)
        def _():
            for i in range(1, 16):
                loss_copy(i).start()

        mine = pl.ds(pl.multiple_of(c * HB, HB), HB)
        theirs = pl.ds(pl.multiple_of((1 - c) * HB, HB), HB)

        def exchange(b):
            sl = b % 2
            return [pltpu.make_async_remote_copy(p.at[sl, theirs, :], r, sxs.at[sl, i], sxr.at[sl, i],
                                                 device_id=(e, partner), device_id_type=MESH)
                    for i, (p, r) in enumerate(((p1, r1), (p2, r2)))]

        def sent(b):
            for i, f in enumerate((f1, f2)):
                for sem in (sscw, ssccw, ssl):
                    pltpu.make_async_copy(f.at[b % NS], (fw1, fw2)[i].at[0], sem.at[i, b % NS]).wait()

        def finish(b):
            sl = b % 2
            fs = b % NS
            for cp in exchange(b):
                cp.wait()

            @pl.when(b >= NS)
            def _():
                sent(b)
            f1[fs] = (p1[sl, mine, :] + r1[...]).T
            f2[fs] = p2[sl, mine, :] + r2[...]

            @pl.when(b < NB - 1)
            def _():
                pl.semaphore_signal(free, 1, device_id=(e, partner), device_id_type=MESH)
            for i, (f, ot, own) in enumerate(((f1, ot1, sf1), (f2, ot2, sf2))):
                def send(dst, to, sems, k):
                    pltpu.make_async_remote_copy(f.at[fs], dst, sems.at[i, fs], rn.at[k, i],
                                                 device_id=(to, tcore), device_id_type=MESH).start()

                for half, (on, on_sems, off, off_sems) in enumerate(((nxt, sscw, prv, ssccw), (prv, ssccw, nxt, sscw))):
                    @pl.when(c == half)
                    def _():
                        if i == 0:
                            send(fw1.at[b], on, on_sems, 0)
                        else:
                            @pl.when(b < NB - NL)
                            def _():
                                send(fw2.at[b], on, on_sems, 0)

                            @pl.when(b >= NB - NL)
                            def _():
                                send(fw3.at[b - (NB - NL)], on, on_sems, 0)
                        send(ot.at[b], off, off_sems, 1)

                @pl.when(c == owner)
                def _():
                    pltpu.make_async_copy(f.at[fs], own.at[c, b], ssl.at[i, fs]).start()

                @pl.when(c != owner)
                def _():
                    pltpu.make_async_remote_copy(f.at[fs], own.at[c, b], ssl.at[i, fs], rd.at[i],
                                                 device_id=(e, tcore), device_id_type=MESH).start()

        def block(b, z):
            sl = b % 2
            wwait(b, 1)

            @pl.when(b < NB - 1)
            def _():
                wwait(b + 1, 0)
                wload(b + 1, 1)

            @pl.when(b < NB - 2)
            def _():
                wload(b + 2, 0)

            def chunk(q, z2):
                @pl.when(b == 0)
                def _():
                    @pl.when(q == 0)
                    def _():
                        for i in range(2 * PQ, NP - PQ):
                            start_load(i)

                    @pl.when(q == NQ - 2)
                    def _():
                        for i in range(NP - PQ, NP):
                            start_load(i)
                    for i in range(PQ):
                        for cp in load(PQ * q + i):
                            cp.wait()

                part = pl.ds(pl.multiple_of(q * (D // NQ), D // NQ), D // NQ)
                wt[1 - sl, :, part] = wb1[1 - sl, part, :].T
                h = [hview(PQ * q + i) for i in range(PQ)]
                g = [gview(PQ * q + i) for i in range(PQ)]
                tiles = [(i, _t(k)) for i in range(PQ) for k in range(TP // FC)]
                groups = [tiles[i:i + GT] for i in range(0, len(tiles), GT)]
                done = {}

                def recompute(i, rs):
                    ut = _dot_t(wt[sl], h[i][rs, :])
                    qt = _dot_t(wb2[sl], g[i][rs, :])
                    th, hu, t2 = _act(ut.astype(BF16).astype(F32))
                    return (_dgelu(th, hu, t2) * qt).astype(BF16), (hu + hu * th).astype(BF16)

                def accumulate(m, n):
                    for p, k, right in ((p1, 0, h), (p2, 1, g)):
                        old = p[sl, :, _t(n)]
                        if m == 0:
                            old = jnp.where(q == 0, 0.0, old)
                        p[sl, :, _t(n)] = old + _sum(_dot(v[k], right[i][rs, _t(n)])
                                                     for v, (i, rs) in zip(done[m], groups[m]))

                for m in range(len(groups) + 1):
                    done[m] = []
                    for k in range(GT):
                        if m < len(groups):
                            done[m].append(recompute(*groups[m][k]))
                        if m > 0:
                            for n in range(k * ND // GT, (k + 1) * ND // GT):
                                accumulate(m - 1, n)

                @pl.when(jnp.logical_and(q == 0, b > 0))
                def _():
                    finish(b - 1)
                return z2

            lax.fori_loop(0, NQ, chunk, 0)

            @pl.when(b > 0)
            def _():
                pl.semaphore_wait(free, 1)
            for cp in exchange(b):
                cp.start()
            return z

        lax.fori_loop(0, NB, block, 0)
        finish(NB - 1)
        for b in range(NB - NS, NB):
            sent(b)

    pl.run_scoped(grads, pltpu.VMEM((2, D, BC), BF16), pltpu.VMEM((2, BC, D), BF16), pltpu.VMEM((2, BC, D), BF16),
                  pltpu.VMEM((2, BC, D), F32), pltpu.VMEM((2, BC, D), F32),
                  pltpu.VMEM((NS, D, HB), F32), pltpu.VMEM((NS, HB, D), F32))


    for i, ot in enumerate((ot1, ot2)):
        for k in range(2):
            pltpu.make_async_copy(ot, ot, rn.at[k, i]).wait()

        @pl.when(c == owner)
        def _():
            pltpu.make_async_copy(ot, ot, rd.at[i]).wait()

    for j in range(2):
        @pl.when(2 * c + j != e)
        def _():
            shipped(j)

    @pl.when(c == owner)
    def _():
        for i in range(2):
            wl_copy(i).wait_send()

    @pl.when(last)
    def _():
        for i in range(1, 16):
            loss_copy(i).wait_send()

    for i in range(4):
        @pl.when(jnp.logical_not(jnp.logical_and(last, e == i)))
        def _():
            pltpu.make_async_remote_copy(lt.at[i], lt.at[i], slt.at[0], rlt.at[i],
                                         device_id=(e, s), device_id_type=MESH).wait_recv()
    oloss[0, 0] = jnp.sum((lt[0] + lt[1]) + (lt[2] + lt[3])) * (0.5 * inv)


def _call(x, t, w1, w2, inv):
    hbm = pl.BlockSpec(memory_space=pl.ANY)
    dma = pltpu.SemaphoreType.DMA
    vmem = pltpu.VMEM
    half1 = jax.ShapeDtypeStruct((NB, D, HB), F32)
    half2 = jax.ShapeDtypeStruct((NB, HB, D), F32)
    out = pl.pallas_call(
        functools.partial(_kernel, inv),
        name="train_step",
        out_shape=(
            half1,
            jax.ShapeDtypeStruct((NB - NL, HB, D), F32),
            jax.ShapeDtypeStruct((NL, HB, D), F32),
            half1, half2,
            jax.ShapeDtypeStruct((2, NB, D, HB), F32),
            jax.ShapeDtypeStruct((2, NB, HB, D), F32),
            jax.ShapeDtypeStruct((1, 1), F32),
            jax.ShapeDtypeStruct((2, TOK, D), BF16),
            jax.ShapeDtypeStruct((2, TOK, D), BF16),
            jax.ShapeDtypeStruct((D, FF), BF16),
            jax.ShapeDtypeStruct((FF, D), BF16),
            jax.ShapeDtypeStruct((2, NK, R, FF), BF16),
        ),
        in_specs=[hbm] * 4,
        out_specs=(hbm,) * 7 + (pl.BlockSpec(memory_space=pltpu.SMEM),) + (hbm,) * 5,
        scratch_shapes=[
            vmem((2, D, FF), BF16), vmem((2, FF, D), BF16),
            vmem((NK, R, D), BF16), vmem((NK, R, D), BF16), vmem((NR, R, D), BF16),
            vmem((HB, D), F32), vmem((HB, D), F32),
            vmem((8, D), F32), vmem((4, 8, 128), F32),
            dma((4,)), dma((NK,)), dma((NK,)), dma((2, 2)), dma, dma,
            dma((NR,)), dma((2,)), dma((2, NK // SPG)), dma((2, NK // SPG)), dma((2,)), dma((2,)),
            dma((2, NP)), dma((2, 2)), dma((2, 2)), dma((2, 2)),
            dma((2, NS)), dma((2, NS)), dma((2, NS)), dma((2, 2)), dma((2,)),
            dma((16,)), dma((4,)), pltpu.SemaphoreType.REGULAR,
        ],
        compiler_params=pltpu.CompilerParams(has_side_effects=True, vmem_limit_bytes=VMEM_LIMIT),
    )(x, t, w1, w2)
    return out[:8]


def _place():
    e = lax.axis_index('dp')
    c = lax.axis_index('pp') % 2
    zz = e // 2
    yy = e % 2
    nxt = 2 * yy + 1 - zz
    prv = 2 * (1 - yy) + zz
    cw = prv // 2 == c
    return e, c, zz, yy, jnp.where(cw, prv, nxt) % 2, jnp.where(cw, 0, 1)


def _region(i, o, j, b, half):
    cs = pl.ds(pl.multiple_of(b * BC + half * HB, HB), HB)
    return o.at[j, :, cs] if i == 0 else o.at[j, cs, :]


def _mover(i, buf, si, so):
    def move(src, dst_of):
        n = src.shape[0]
        ns = min(buf.shape[0], n)
        ahead = n if n == ns else ns // 2

        def into(b):
            return pltpu.make_async_copy(src.at[b], buf.at[b % ns], si.at[b % ns])

        def out(b):
            return pltpu.make_async_copy(buf.at[b % ns], dst_of(b), so.at[b % ns])

        for b in range(ahead):
            into(b).start()

        def step(b, z):
            into(b).wait()
            out(b).start()

            if ahead < n:
                @pl.when(b + ahead < n)
                def _():
                    @pl.when(b >= ahead)
                    def _():
                        out(b - ahead).wait()
                    into(b + ahead).start()
            return z

        lax.fori_loop(0, n, step, 0)
        for b in range(n - ns, n):
            out(b).wait()

    return move


def _direct_kernel(i, *refs):
    *fw, ot, sf, o, buf, si, so = refs
    e, c, _, _, jn, half = _place()
    move = _mover(i, buf, si, so)
    first = 0
    for part in fw:
        move(part, lambda b, first=first: _region(i, o, jn, first + b, half))
        first += part.shape[0]
    move(ot, lambda b: _region(i, o, jn, b, 1 - half))

    @pl.when(c == e // 2)
    def _():
        for h in range(2):
            move(sf.at[h], lambda b: _region(i, o, e % 2, b, h))


def _onward_kernel(first, i, o_in, za, yb, *refs):
    *_, o, buf, si, so = refs
    e, c, zz, yy, jn, _ = _place()
    move = _mover(i, buf, si, so)

    @pl.when(c != e // 2)
    def _():
        h = jnp.where(zz == yy, 0, 1)
        move(za, lambda b: _region(i, o, 1 - jn, first + b, h))
        move(yb, lambda b: _region(i, o, 1 - jn, first + b, 1 - h))


def _placing(body, i, name, args, alias):
    hbm = pl.BlockSpec(memory_space=pltpu.HBM)
    tile = (D, HB) if i == 0 else (HB, D)
    shape = (2, D, FF) if i == 0 else (2, FF, D)
    return pl.pallas_call(
        functools.partial(body, i),
        name=name,
        out_shape=jax.ShapeDtypeStruct(shape, F32),
        in_specs=[hbm] * len(args),
        out_specs=hbm,
        input_output_aliases=alias,
        scratch_shapes=[pltpu.VMEM((16,) + tile, F32), pltpu.SemaphoreType.DMA((16,)), pltpu.SemaphoreType.DMA((16,))],
        cost_estimate=pl.CostEstimate(flops=20_000_000_000, bytes_accessed=64 << 20, transcendentals=0),
        compiler_params=pltpu.CompilerParams(vmem_limit_bytes=VMEM_LIMIT),
    )(*args)


def _onward_pairs(npp):
    pairs = ([], [])
    for q in range(4):
        z, y = divmod(q, 2)
        nxt, prv = 2 * y + 1 - z, 2 * (1 - y) + z
        for c in range(2):
            to = nxt if prv // 2 == c else prv
            for xx in range(npp // 2):
                pairs[0 if to % 2 == y else 1].append((q * npp + 2 * xx + c, to * npp + 2 * xx + c))
    return pairs


def solution(mesh):
    ndp = mesh.shape['dp']
    along = _onward_pairs(mesh.shape['pp'])

    def body(x, t, w1, w2):
        nm, tok, d = x.shape
        fw1, fw2, fw3, ot1, ot2, sf1, sf2, loss = _call(x, t, w1[0], w2[0], 1.0 / (nm * tok * ndp * d))
        parts = ((0, 0, fw1), (1, 0, fw2), (1, NB - NL, fw3))
        on = [[lax.ppermute(fw, ('dp', 'pp'), p) for p in along] for _, _, fw in parts]
        out = [_placing(_direct_kernel, 0, "direct", (fw1, ot1, sf1), {}),
               _placing(_direct_kernel, 1, "direct", (fw2, fw3, ot2, sf2), {})]
        for (i, start, _), got in zip(parts, on):
            after = (out[0],) if start else ()
            out[i] = _placing(functools.partial(_onward_kernel, start), i, "onward", (out[i], *got, *after), {0: 0})
        return out[0][None], out[1][None], loss[0, 0]

    return jax.shard_map(body, mesh=mesh,
                         in_specs=(P(None, 'dp', None), P(None, 'dp', None), P('pp'), P('pp')),
                         out_specs=(P('pp'), P('pp'), P()), check_vma=False)
```
